32 devices in a mesh: lat: 4 (over z), lon: 8 (over y, x, core).
Axes of the slice: x: 2, y: 2, z: 4, core: 2. Of those that a mesh axis runs over, the one named last changes fastest.
Arguments:
- fields: float32 [32, 2880, 384], P('lat', 'lon'), may hold values from -6 to 6
- cutoff: int32 [32], P('lat'), may hold values from 1 to 1395, as said below
Outputs:
- filtered: float32 [32, 2880, 384], P('lat', 'lon')
The draws below stay inside these ranges and needn't reach their ends.
Inputs may be any that keep to these rules, and one draw needn't show every extreme that they name: cutoff[g] lies between 1 and 1 + (1439)(2 p + 1) // 32, where p is the number of rows between row g and the nearer pole; this ceiling grows from the pole rows to the equator.
All inputs are finite; a program needn't handle non-finite values.
Results may differ from the reference program's by a relative error of at most 0.0003.
Values sent between devices are 32-bit elements; how exact they have to be, the bound alone decides.
A program may use at most 64 MiB of HBM per device.

```python
import jax
import jax.numpy as jnp
from jax import lax

NLON = 2880
FIELDS = 6
LEVELS = 64
NLAT = 32


def draw_cutoff(key, part):
    row_id = jnp.arange(NLAT, dtype=jnp.int32)
    pole_rows = jnp.minimum(row_id, NLAT - 1 - row_id)
    highest_cut = 1 + (NLON // 2 - 1) * (2 * pole_rows + 1) // NLAT
    drawn = jax.random.randint(key, (NLAT,), 1, highest_cut + 1, dtype=jnp.int32)
    drawn = drawn.at[NLAT // 2].set(highest_cut[NLAT // 2])
    drawn = drawn.at[NLAT - 1].set(1)
    return drawn


def block_levels(key, dims, split, smallest, top_value):
    level = 1.0
    for dim, shards_of in split:
        draws = jax.random.uniform(jax.random.fold_in(jax.random.fold_in(key, 6), dim), (shards_of,), jnp.float32, smallest / len(split), top_value / len(split))
        level = level * jnp.repeat(jnp.exp(draws), dims[dim] // shards_of).reshape((-1,) + (1,) * (len(dims) - 1 - dim))
    return level


def scatter_about(own_key, shape, scale, limit, split=(), kind=jnp.bfloat16):
    gain = block_levels(own_key, shape, split, -0.22, 0.18) if split else 1.0
    array = jax.random.normal(own_key, shape, jnp.float32) * scale * gain
    return jnp.minimum(jnp.maximum(array, -limit), limit).astype(kind)


def setup_inputs(seed: int = 0) -> dict:
    streams_of = jax.random.split(jax.random.key(seed), 3)
    fields = scatter_about(streams_of[0], (NLAT, NLON, FIELDS * LEVELS), 1.0, 6.0, ((0, 4), (1, 8)), jnp.float32)
    cutoff = draw_cutoff(jax.random.fold_in(streams_of[2], 71), 0)
    return {"fields": fields, "cutoff": cutoff}


def polar_mask(total_rows):
    latitude_row = jnp.arange(total_rows, dtype=jnp.int32)
    offset_twice = jnp.abs(2 * latitude_row + 1 - total_rows)
    return offset_twice * 5 > 2 * total_rows


def damping_row(cutoff_row, length):
    wavenumber = jnp.arange(length // 2 + 1, dtype=jnp.int32)
    cutoff_float = cutoff_row.astype(jnp.float32)
    wave_float = jnp.maximum(wavenumber, 1).astype(jnp.float32)
    ratio_value = jnp.sin(jnp.pi * cutoff_float / length) / jnp.sin(jnp.pi * wave_float / length)
    return jnp.where(wavenumber <= cutoff_row, 1.0, ratio_value * ratio_value).astype(jnp.float32)


def reference(fields, cutoff):
    total_rows = fields.shape[0]
    length = fields.shape[1]
    polar_rows = polar_mask(total_rows)

    def filter_row(packed):
        row_field, row_cutoff, row_polar = packed
        spectrum = jnp.fft.rfft(row_field, axis=0)
        scaled = spectrum * damping_row(row_cutoff, length)[:, None]
        smoothed = jnp.fft.irfft(scaled, n=length, axis=0).astype(jnp.float32)
        return jnp.where(row_polar, smoothed, row_field)

    return lax.map(filter_row, (fields, cutoff, polar_rows))
```

```python
import functools
import math

import jax
import jax.numpy as jnp
import ml_dtypes
import numpy as np
from jax import lax
from jax.experimental import pallas as pl
from jax.experimental.pallas import tpu as pltpu
from jax.sharding import PartitionSpec as P

RADIX = 8


def split_np(a):
    hi = a.astype(ml_dtypes.bfloat16)
    lo = (a - hi.astype(np.float64)).astype(ml_dtypes.bfloat16)
    return hi, lo


def fourier_table(sub, padded):
    turn = np.outer(np.arange(sub), np.arange(sub)) % sub
    angle = 2.0 * np.pi * turn / sub
    both = np.concatenate([np.cos(angle), np.sin(angle)], axis=0)
    both = np.pad(both, ((0, 0), (0, padded - sub)))
    hi, lo = split_np(both)
    return np.concatenate([hi, lo, hi], axis=1)


def twist_table(sub, length):
    b = np.arange(RADIX // 2 + 1)
    angle = 2.0 * np.pi * np.outer(np.arange(sub), b) / length
    return np.concatenate([np.cos(angle), np.sin(angle)], axis=1).astype(np.float32)


def gain_table(cut, sub, length):
    half = RADIX // 2
    wave = np.arange(sub)[:, None] * RADIX + np.arange(half + 1)[None, :]
    folded = np.minimum(wave, length - wave)
    scale = np.where((np.arange(half + 1) % half) == 0, 1.0, 2.0)[None, :] / length
    inverse_sine = 1.0 / np.sin(np.pi * np.maximum(folded, 1) / length)
    ratio = jnp.sin(cut * jnp.float32(math.pi / length)) * inverse_sine.astype(np.float32)
    gain = jnp.where(folded.astype(np.float32) <= cut, 1.0, ratio * ratio)
    return gain * scale.astype(np.float32)


def three(table, z, padded):
    pad = padded - z.shape[0]
    if pad:
        z = jnp.concatenate([z, jnp.zeros((pad, z.shape[1]), z.dtype)], axis=0)
    hi = z.astype(jnp.bfloat16)
    lo = (z - hi.astype(jnp.float32)).astype(jnp.bfloat16)
    return jnp.dot(table, jnp.concatenate([hi, hi, lo], axis=0), preferred_element_type=jnp.float32)


def filter_kernel(sub, padded, flag_ref, x_ref, table_ref, twist_ref, gain_ref, y_ref):
    width = x_ref.shape[-1]
    half = RADIX // 2
    r = math.sqrt(0.5)

    @pl.when(flag_ref[0] == 0)
    def _():
        y_ref[...] = x_ref[...]

    @pl.when(flag_ref[0] != 0)
    def _():
        x = [x_ref[pl.ds(j * sub, sub), :] for j in range(RADIX)]
        s = [x[j] + x[j + 4] for j in range(4)]
        d = [x[j] - x[j + 4] for j in range(4)]
        s02, s13 = s[0] + s[2], s[1] + s[3]
        p, q = r * (d[1] - d[3]), r * (d[1] + d[3])
        spectra = [
            (s02 + s13, None),
            (d[0] + p, -(d[2] + q)),
            (s[0] - s[2], s[3] - s[1]),
            (d[0] - p, d[2] - q),
            (s02 - s13, None),
        ]
        table = table_ref[...]
        back = []
        for b in range(half + 1):
            re, im = spectra[b]
            gain = gain_ref[:, b : b + 1]
            if b == 0:
                f = three(table, re, padded)
                g = three(table, jnp.concatenate([f[:sub] * gain, f[sub:] * gain], axis=1), padded)
                back.append((g[:sub, :width] + g[sub:, width:], None))
                continue
            c = twist_ref[:, b : b + 1]
            t = twist_ref[:, half + 1 + b : half + 2 + b]
            if im is None:
                zr, zi = re * c, -(re * t)
            else:
                zr, zi = re * c + im * t, im * c - re * t
            f = three(table, jnp.concatenate([zr, zi], axis=1), padded)
            fr = (f[:sub, :width] + f[sub:, width:]) * gain
            fi = (f[:sub, width:] - f[sub:, :width]) * gain
            g = three(table, jnp.concatenate([fr, fi], axis=1), padded)
            gr = g[:sub, :width] - g[sub:, width:]
            gi = g[:sub, width:] + g[sub:, :width]
            back.append((gr * c - gi * t, gr * t + gi * c))
        y0, y4 = back[0][0], back[4][0]
        (a1, b1), (a2, b2), (a3, b3) = back[1:4]
        e, o = y0 + y4, y0 - y4
        u, v = a1 + a3, b1 - b3
        w, z = r * (a1 - a3), r * (b1 + b3)
        outs = {
            0: e + a2 + u,
            4: e + a2 - u,
            2: e - a2 - v,
            6: e - a2 + v,
            1: o - b2 + w - z,
            5: o - b2 - w + z,
            3: o + b2 - w - z,
            7: o + b2 + w + z,
        }
        for j in range(RADIX):
            y_ref[pl.ds(j * sub, sub), :] = outs[j]


def filter_row(row, cut, polar):
    length, channels = row.shape
    sub = length // RADIX
    padded = -(-sub // 128) * 128
    block = 128 if channels % 128 == 0 else channels
    table = fourier_table(sub, padded)
    twist = twist_table(sub, length)
    gain = gain_table(cut, sub, length)
    whole = lambda a: pl.BlockSpec(a.shape, lambda i: (0, 0))
    return pl.pallas_call(
        functools.partial(filter_kernel, sub, padded),
        out_shape=jax.ShapeDtypeStruct(row.shape, row.dtype),
        grid=(channels // block,),
        in_specs=[
            pl.BlockSpec(memory_space=pltpu.SMEM),
            pl.BlockSpec((length, block), lambda i: (0, i)),
            whole(table),
            whole(twist),
            whole(gain),
        ],
        out_specs=pl.BlockSpec((length, block), lambda i: (0, i)),
        compiler_params=pltpu.CompilerParams(vmem_limit_bytes=56 * 1024 * 1024),
        name="row_filter",
    )(polar.reshape(1), row, table, twist, gain)


def polar_table(row_count, band_count):
    total_rows = row_count * band_count
    row_ids = np.arange(total_rows)
    polar_flags = (np.abs(2 * row_ids + 1 - total_rows) * 5 > 2 * total_rows).astype(np.int32)
    return polar_flags.reshape(band_count, row_count)


def local(fields, cutoff):
    rows, segment, channels = fields.shape
    ring = lax.axis_size("lon")
    groups = max(1, ring // rows)
    each = rows * groups // ring
    width = channels // groups
    assert each * ring == rows * groups and width * groups == channels
    pieces = fields
    if groups > 1:
        pieces = fields.reshape(rows, segment, groups, width).transpose(0, 2, 1, 3)
    pieces = pieces.reshape(ring, each, segment, width)
    whole = lax.all_to_all(pieces, "lon", 0, 0, tiled=True)
    first_row = lax.axis_index("lon") * each // groups
    flags = jnp.asarray(polar_table(rows, lax.axis_size("lat")))[lax.axis_index("lat")]
    done = []
    for i in range(each):
        row = whole[:, i].reshape(ring * segment, width)
        cut = lax.dynamic_index_in_dim(cutoff, first_row + i, 0, False).astype(jnp.float32)
        flag = lax.dynamic_index_in_dim(flags, first_row + i, 0, False)
        done.append(filter_row(row, cut, flag).reshape(ring, segment, width))
    back = lax.all_to_all(jnp.stack(done, axis=1), "lon", 0, 0, tiled=True)
    if groups > 1:
        back = back.reshape(rows, groups, segment, width).transpose(0, 2, 1, 3)
    return back.reshape(rows, segment, channels)


def solution(mesh):
    return jax.shard_map(
        local,
        mesh=mesh,
        in_specs=(P("lat", "lon", None), P("lat")),
        out_specs=P("lat", "lon", None),
        check_vma=False,
    )
```

```python
import functools
import math

import jax
import jax.numpy as jnp
import ml_dtypes
import numpy as np
from jax import lax
from jax.experimental import pallas as pl
from jax.experimental.pallas import tpu as pltpu
from jax.sharding import PartitionSpec as P

RADIX = 8


def split_np(a):
    hi = a.astype(ml_dtypes.bfloat16)
    lo = (a - hi.astype(np.float64)).astype(ml_dtypes.bfloat16)
    return hi, lo


def fourier_table(sub, padded):
    turn = np.outer(np.arange(sub), np.arange(sub)) % sub
    angle = 2.0 * np.pi * turn / sub
    both = np.concatenate([np.cos(angle), np.sin(angle)], axis=0)
    both = np.pad(both, ((0, 0), (0, padded - sub)))
    hi, lo = split_np(both)
    return np.concatenate([hi, lo, hi], axis=1)


def twist_table(sub, length):
    b = np.arange(RADIX // 2 + 1)
    angle = 2.0 * np.pi * np.outer(np.arange(sub), b) / length
    return np.concatenate([np.cos(angle), np.sin(angle)], axis=1).astype(np.float32)


def gain_table(cut, sub, length):
    half = RADIX // 2
    wave = np.arange(sub)[:, None] * RADIX + np.arange(half + 1)[None, :]
    folded = np.minimum(wave, length - wave)
    scale = np.where((np.arange(half + 1) % half) == 0, 1.0, 2.0)[None, :] / length
    inverse_sine = 1.0 / np.sin(np.pi * np.maximum(folded, 1) / length)
    ratio = jnp.sin(cut * jnp.float32(math.pi / length)) * inverse_sine.astype(np.float32)
    gain = jnp.where(folded.astype(np.float32) <= cut, 1.0, ratio * ratio)
    return gain * scale.astype(np.float32)


def three(table, z, padded):
    pad = padded - z.shape[0]
    if pad:
        z = jnp.concatenate([z, jnp.zeros((pad, z.shape[1]), z.dtype)], axis=0)
    hi = z.astype(jnp.bfloat16)
    lo = (z - hi.astype(jnp.float32)).astype(jnp.bfloat16)
    return jnp.dot(table, jnp.concatenate([hi, hi, lo], axis=0), preferred_element_type=jnp.float32)


def filter_row(sub, padded, x_ref, table_ref, twist_ref, gains, y_ref):
    width = x_ref.shape[-1]
    half = RADIX // 2
    r = math.sqrt(0.5)
    x = [x_ref[pl.ds(j * sub, sub), :] for j in range(RADIX)]
    s = [x[j] + x[j + 4] for j in range(4)]
    d = [x[j] - x[j + 4] for j in range(4)]
    s02, s13 = s[0] + s[2], s[1] + s[3]
    p, q = r * (d[1] - d[3]), r * (d[1] + d[3])
    spectra = [
        (s02 + s13, None),
        (d[0] + p, -(d[2] + q)),
        (s[0] - s[2], s[3] - s[1]),
        (d[0] - p, d[2] - q),
        (s02 - s13, None),
    ]
    table = table_ref[...]
    back = []
    for b in range(half + 1):
        re, im = spectra[b]
        gain = gains[:, b : b + 1]
        if b == 0:
            f = three(table, re, padded)
            g = three(table, jnp.concatenate([f[:sub] * gain, f[sub:] * gain], axis=1), padded)
            back.append((g[:sub, :width] + g[sub:, width:], None))
            continue
        c = twist_ref[:, b : b + 1]
        t = twist_ref[:, half + 1 + b : half + 2 + b]
        if im is None:
            zr, zi = re * c, -(re * t)
        else:
            zr, zi = re * c + im * t, im * c - re * t
        f = three(table, jnp.concatenate([zr, zi], axis=1), padded)
        fr = (f[:sub, :width] + f[sub:, width:]) * gain
        fi = (f[:sub, width:] - f[sub:, :width]) * gain
        g = three(table, jnp.concatenate([fr, fi], axis=1), padded)
        gr = g[:sub, :width] - g[sub:, width:]
        gi = g[:sub, width:] + g[sub:, :width]
        back.append((gr * c - gi * t, gr * t + gi * c))
    y0, y4 = back[0][0], back[4][0]
    (a1, b1), (a2, b2), (a3, b3) = back[1:4]
    e, o = y0 + y4, y0 - y4
    u, v = a1 + a3, b1 - b3
    w, z = r * (a1 - a3), r * (b1 + b3)
    outs = {
        0: e + a2 + u,
        4: e + a2 - u,
        2: e - a2 - v,
        6: e - a2 + v,
        1: o - b2 + w - z,
        5: o - b2 - w + z,
        3: o + b2 - w - z,
        7: o + b2 + w + z,
    }
    for j in range(RADIX):
        y_ref[pl.ds(j * sub, sub), :] = outs[j]


def split_table(a):
    hi = a.astype(jnp.bfloat16)
    lo = (a - hi.astype(jnp.float32)).astype(jnp.bfloat16)
    return jnp.concatenate([hi, lo, hi], axis=1)


def snap(a):
    return (np.round(a * 2.0**22) / 2.0**22).astype(np.float32)


def toeplitz(symbol, sub):
    line = np.fft.ifft(symbol).real
    index = np.arange(sub)
    return line[(index[:, None] - index[None, :]) % symbol.shape[0]]


class Plan:
    def __init__(self, rows, segment, channels, ring, bands):
        length, total = segment * ring, rows * bands
        self.width = 128 if channels % 128 == 0 else channels
        blocks = channels // self.width
        row_ids = np.arange(total)
        polar = np.abs(2 * row_ids + 1 - total) * 5 > 2 * total
        poles = np.minimum(row_ids, total - 1 - row_ids)
        count = int(poles[polar].max()) + 1
        cuts = 1 + (length // 2 - 1) * (2 * np.arange(count) + 1) // total
        full = -(-segment // 8) * 8
        ranks = [min(full, -(-((2 * int(c) + 1) // ring + 21) // 8) * 8) for c in cuts]
        self.rank = max(ranks)
        self.rank_pad = -(-self.rank // 128) * 128
        self.sub_pad = -(-segment // 128) * 128
        wave = np.arange(length)
        folded = np.minimum(wave, length - wave)
        sine = np.sin(np.pi * np.maximum(folded, 1) / length) ** 2
        spot = np.arange(segment)
        probe = np.cos(1.0 + 0.37 * spot * spot)
        self.basis = np.zeros((count, segment, self.rank_pad), np.float32)
        self.basis_t = np.zeros((count, self.rank, self.sub_pad), np.float32)
        self.rest = np.zeros((count, segment, self.sub_pad), np.float32)
        top = np.sin(np.pi * cuts / length) ** 2
        self.top = top.astype(np.float32)
        for p in range(count):
            take = min(ranks[p], segment)
            side = spot[1:] * (segment - spot[1:]) / 2.0
            band = (cuts[p] + 0.5) / length
            tri = np.diag(((segment - 1) / 2.0 - spot) ** 2 * np.cos(2.0 * np.pi * band))
            tri = tri + np.diag(side, 1) + np.diag(side, -1)
            vectors = np.linalg.eigh(tri)[1][:, ::-1][:, :take]
            vectors = vectors * np.where(probe @ vectors < 0, -1.0, 1.0)
            basis = snap(vectors)
            if take == segment:
                basis = np.eye(segment, dtype=np.float32)
            self.basis[p, :, :take] = basis
            self.basis_t[p, :take, :segment] = basis.T
            near = toeplitz(np.minimum(1.0 / sine, 1.0 / top[p]) * top[p], segment)
            wide = basis.astype(np.float64)
            self.rest[p, :, :segment] = snap(near - wide @ (wide.T @ near @ wide) @ wide.T)
        slots = -(-rows * blocks // ring)
        self.slots = slots
        self.row_pole = np.zeros((bands, rows), np.int32)
        self.row_on = np.zeros((bands, rows), np.int32)
        self.dest = np.zeros((bands, rows, blocks), np.int32)
        self.offset = np.zeros((bands, rows, blocks), np.int32)
        self.unit_row = np.zeros((bands, ring, slots), np.int32)
        self.unit_pole = np.zeros((bands, ring, slots), np.int32)
        self.unit_on = np.zeros((bands, ring, slots), np.int32)
        self.unit_offset = np.zeros((bands, ring, slots), np.int32)
        self.height = 8
        for b in range(bands):
            ids = np.arange(rows) + b * rows
            self.row_on[b] = polar[ids]
            self.row_pole[b] = np.where(polar[ids], poles[ids], 0)
            held = [[] for _ in range(ring)]
            load = [0] * ring
            units = [(ranks[poles[ids[i]]], i, c) for i in range(rows) if polar[ids[i]] for c in range(blocks)]
            for rank, i, c in sorted(units, key=lambda u: (-u[0], u[1], u[2])):
                d = min((e for e in range(ring) if len(held[e]) < slots), key=lambda e: (load[e], e))
                held[d].append((i, c, rank))
                load[d] += rank
            self.height = max(self.height, max(load))
            for d in range(ring):
                start = 0
                for n, (i, c, rank) in enumerate(sorted(held[d])):
                    self.dest[b, i, c], self.offset[b, i, c] = d, start
                    self.unit_row[b, d, n], self.unit_on[b, d, n] = i, 1
                    self.unit_pole[b, d, n], self.unit_offset[b, d, n] = poles[ids[i]], start
                    start += rank


def pack_kernel(plan, pole, on, dest, offset, x_ref, basis_ref, out_ref, hold):
    i = pl.program_id(0)
    width, blocks = plan.width, dest.shape[0] // on.shape[0]

    @pl.when(i == 0)
    def _():
        hold[...] = jnp.zeros_like(hold)

    @pl.when(on[i] != 0)
    def _():
        z = three(split_table(basis_ref[0]), x_ref[0], plan.sub_pad)
        for c in range(blocks):
            at = pl.multiple_of(offset[i * blocks + c], 8)
            hold[dest[i * blocks + c], pl.ds(at, plan.rank), :] = z[:, c * width : (c + 1) * width]

    @pl.when(i == pl.num_programs(0) - 1)
    def _():
        out_ref[...] = hold[:, : plan.height, :]


def unit_kernel(plan, sub, padded, pole, on, offset, w_ref, basis_ref, basis_t_ref, table_ref, twist_ref, gain_ref, out_ref, came, hold, x_row, y_row):
    i = pl.program_id(0)
    ring, width = w_ref.shape[0], plan.width
    segment = basis_ref.shape[1]

    @pl.when(i == 0)
    def _():
        hold[...] = jnp.zeros_like(hold)
        came[:, : plan.height, :] = w_ref[...]
        came[:, plan.height :, :] = jnp.zeros((ring, plan.rank, width), jnp.float32)

    @pl.when(on[i] != 0)
    def _():
        at = pl.multiple_of(offset[i], 8)
        z = jnp.concatenate([came[j, pl.ds(at, plan.rank), :] for j in range(ring)], axis=1)
        x = three(split_table(basis_ref[0]), z, plan.rank_pad)
        for j in range(ring):
            x_row[pl.ds(j * segment, segment), :] = x[:, j * width : (j + 1) * width]
        filter_row(sub, padded, x_row, table_ref, twist_ref, gain_ref[0], y_row)
        y = jnp.concatenate([y_row[pl.ds(j * segment, segment), :] for j in range(ring)], axis=1)
        z = three(split_table(basis_t_ref[0]), y, plan.sub_pad)
        for j in range(ring):
            hold[j, pl.ds(at, plan.rank), :] = z[:, j * width : (j + 1) * width]

    @pl.when(i == pl.num_programs(0) - 1)
    def _():
        out_ref[...] = hold[:, : plan.height, :]


def unpack_kernel(plan, pole, on, dest, offset, w_ref, x_ref, scale_ref, basis_ref, rest_ref, y_ref, came):
    i = pl.program_id(0)
    ring, width = w_ref.shape[0], plan.width
    blocks = dest.shape[0] // on.shape[0]

    @pl.when(i == 0)
    def _():
        came[:, : plan.height, :] = w_ref[...]
        came[:, plan.height :, :] = jnp.zeros((ring, plan.rank, width), jnp.float32)

    @pl.when(on[i] == 0)
    def _():
        y_ref[...] = x_ref[...]

    @pl.when(on[i] != 0)
    def _():
        parts = []
        for c in range(blocks):
            at = pl.multiple_of(offset[i * blocks + c], 8)
            parts.append(came[dest[i * blocks + c], pl.ds(at, plan.rank), :])
        coef = jnp.concatenate(parts, axis=1)
        low = three(split_table(basis_ref[0]), coef, plan.rank_pad)
        high = three(split_table(rest_ref[0]), x_ref[0], plan.sub_pad)
        y_ref[0] = low + high * scale_ref[i]


def local(ring, bands, fields, cutoff):
    rows, segment, channels = fields.shape
    length = ring * segment
    sub = length // RADIX
    padded = -(-sub // 128) * 128
    plan = Plan(rows, segment, channels, ring, bands)
    width, height, rank = plan.width, plan.height, plan.rank
    band, me = lax.axis_index("lat"), lax.axis_index("lon")
    params = pltpu.CompilerParams(vmem_limit_bytes=56 * 1024 * 1024)
    f32 = jnp.float32

    pick = lambda a, *at: functools.reduce(lambda t, n: lax.dynamic_index_in_dim(t, n, 0, False), at, jnp.asarray(a))
    pole, on = pick(plan.row_pole, band), pick(plan.row_on, band)
    dest, offset = pick(plan.dest, band).reshape(-1), pick(plan.offset, band).reshape(-1)
    unit_row, unit_on = pick(plan.unit_row, band, me), pick(plan.unit_on, band, me)
    unit_pole, unit_offset = pick(plan.unit_pole, band, me), pick(plan.unit_offset, band, me)
    cut = cutoff.astype(f32)
    scale = jnp.sin(cut * f32(math.pi / length)) ** 2 / jnp.asarray(plan.top)[pole]
    gains = jnp.stack([gain_table(cut[unit_row[n]], sub, length) for n in range(plan.slots)])

    by_row = pl.BlockSpec((1, segment, channels), lambda i, *s: (i, 0, 0))
    by_pole = lambda a: pl.BlockSpec((1,) + a.shape[1:], lambda i, pole, *s: (pole[i], 0, 0))
    whole = lambda a: pl.BlockSpec(a.shape, lambda i, *s: (0,) * a.ndim)
    sent = jax.ShapeDtypeStruct((ring, height, width), f32)
    buffer = pltpu.VMEM((ring, height + rank, width), f32)

    packed = pl.pallas_call(
        functools.partial(pack_kernel, plan),
        out_shape=sent,
        grid_spec=pltpu.PrefetchScalarGridSpec(
            num_scalar_prefetch=4,
            grid=(rows,),
            in_specs=[by_row, by_pole(plan.basis_t)],
            out_specs=whole(sent),
            scratch_shapes=[buffer],
        ),
        compiler_params=params,
        name="pack",
    )(pole, on, dest, offset, fields, plan.basis_t)
    packed = lax.all_to_all(packed, "lon", 0, 0, tiled=True)
    table = fourier_table(sub, padded)
    twist = twist_table(sub, length)
    packed = pl.pallas_call(
        functools.partial(unit_kernel, plan, sub, padded),
        out_shape=sent,
        grid_spec=pltpu.PrefetchScalarGridSpec(
            num_scalar_prefetch=3,
            grid=(plan.slots,),
            in_specs=[
                whole(sent),
                by_pole(plan.basis),
                by_pole(plan.basis_t),
                whole(table),
                whole(twist),
                pl.BlockSpec((1,) + gains.shape[1:], lambda i, *s: (i, 0, 0)),
            ],
            out_specs=whole(sent),
            scratch_shapes=[buffer, buffer, pltpu.VMEM((length, width), f32), pltpu.VMEM((length, width), f32)],
        ),
        compiler_params=params,
        name="unit_filter",
    )(unit_pole, unit_on, unit_offset, packed, plan.basis, plan.basis_t, table, twist, gains)
    packed = lax.all_to_all(packed, "lon", 0, 0, tiled=True)
    return pl.pallas_call(
        functools.partial(unpack_kernel, plan),
        out_shape=jax.ShapeDtypeStruct(fields.shape, fields.dtype),
        grid_spec=pltpu.PrefetchScalarGridSpec(
            num_scalar_prefetch=4,
            grid=(rows,),
            in_specs=[
                whole(sent),
                by_row,
                pl.BlockSpec(memory_space=pltpu.SMEM),
                by_pole(plan.basis),
                by_pole(plan.rest),
            ],
            out_specs=by_row,
            scratch_shapes=[buffer],
        ),
        compiler_params=params,
        name="unpack",
    )(pole, on, dest, offset, packed, fields, scale, plan.basis, plan.rest)


def solution(mesh):
    return jax.shard_map(
        functools.partial(local, mesh.shape["lon"], mesh.shape["lat"]),
        mesh=mesh,
        in_specs=(P("lat", "lon", None), P("lat")),
        out_specs=P("lat", "lon", None),
        check_vma=False,
    )
```
